32 devices in a mesh: groups: 2 (over y), cells: 8 (over z, x), side: 2 (over core).
Axes of the slice: x: 2, y: 2, z: 4, core: 2. Of those that a mesh axis runs over, the one named last changes fastest.
Arguments:
- datasets: float32 [2, 2000, 8192], P('side', None, ('groups', 'cells')), parts along dimension 2, may hold values from -6 to 6
- sketch: float32 [64, 8192], P(None, ('groups', 'cells')), parts along dimension 1, may hold values from -6 to 6
Outputs:
- factors: float32 [2, 64, 8192], P('side', None, ('groups', 'cells')), parts along dimension 2
The draws below stay inside these ranges and needn't reach their ends.
There are 2 independent parts, one for each index of `groups`. The reference program is written for one: setup_inputs(seed, part) draws one part's arguments, and reference() takes and returns one part's arrays. A program takes and returns all parts, laid end to end along the dimension named above; each array names one. Nothing has to cross between parts.
All inputs are finite; a program needn't handle non-finite values.
Results may differ from the reference program's by a relative error of at most 0.00009.
Values sent between devices are 32-bit elements; how exact they have to be, the bound alone decides.
A program may use at most 64 MiB of HBM per device.

```python
import jax
import jax.numpy as jnp
from jax import lax

G = 2000
K = 64
NCELLS = 4096


def shard_levels(key, dims, cuts, low, top_value):
    level = 1.0
    for dim, shards_of in cuts:
        steps = jax.random.uniform(jax.random.fold_in(jax.random.fold_in(key, 6), dim), (shards_of,), jnp.float32, low / len(cuts), top_value / len(cuts))
        level = level * jnp.repeat(jnp.exp(steps), dims[dim] // shards_of).reshape((-1,) + (1,) * (len(dims) - 1 - dim))
    return level


def scatter_about(stream_key, extent, spread, limit, split=(), kind=jnp.bfloat16):
    loudness = shard_levels(stream_key, extent, split, -0.22, 0.18) if split else 1.0
    entries = jax.random.normal(stream_key, extent, jnp.float32) * spread * loudness
    return jnp.minimum(jnp.maximum(entries, -limit), limit).astype(kind)


def setup_inputs(seed: int = 0, part: int = 0) -> dict:
    key_list = jax.random.split(jax.random.key(seed), 3)
    own_keys = jax.random.split(jax.random.fold_in(key_list[2], part), 3)
    datasets = scatter_about(own_keys[0], (2, G, NCELLS), 1.0, 6.0, ((0, 2), (2, 8)), jnp.float32)
    sketch = scatter_about(own_keys[1], (K, NCELLS), 1.0, 6.0, ((1, 8),), jnp.float32)
    return {"datasets": datasets, "sketch": sketch}


def reference(datasets, sketch):
    high = lax.Precision.HIGHEST
    first = datasets[0]
    second = datasets[1]
    panel = jnp.dot(sketch, second.T, precision=high)
    range_rows = jnp.dot(panel, first, precision=high)
    gram = jnp.dot(range_rows, range_rows.T, precision=high)
    lower = jnp.linalg.cholesky(gram)
    basis = jax.scipy.linalg.solve_triangular(lower, range_rows, lower=True)
    cross = jnp.dot(basis, first.T, precision=high)
    projected = jnp.dot(cross, second, precision=high)
    scale = jnp.sqrt(jnp.float32(NCELLS))
    return jnp.stack([basis * scale, projected / scale])
```

```python
import functools
import math

import jax
import jax.numpy as jnp
from jax import lax
from jax.experimental import pallas as pl
from jax.experimental.pallas import tpu as pltpu
from jax.sharding import PartitionSpec as P

MESH = pl.DeviceIdType.MESH
F32, BF16 = jnp.float32, jnp.bfloat16
HIGHEST = lax.Precision.HIGHEST
NT = (((1,), (1,)), ((), ()))
NN = (((1,), (0,)), ((), ()))


def each(count, body):
    if count <= 8:
        for index in range(count):
            body(index)
    else:
        lax.fori_loop(0, count, lambda index, carry: (body(index), carry)[1], 0)


def halves(value):
    high = value.astype(BF16)
    low = (value - high.astype(F32)).astype(BF16)
    return high, low


def stacked(value):
    return jnp.concatenate(halves(value), axis=0)


def dot3(small, high, low, dims):
    rows = small.shape[0] // 2
    both = lax.dot_general(small, high, dims, preferred_element_type=F32)
    rest = lax.dot_general(small[:rows], low, dims, preferred_element_type=F32)
    return both[:rows] + (both[rows:] + rest)


def inverse_factor(gram):
    k = gram.shape[0]
    row_ids = lax.broadcasted_iota(jnp.int32, gram.shape, 0)
    lanes = lax.broadcasted_iota(jnp.int32, gram.shape, 1)
    start = jnp.where(lanes < k, (lanes == row_ids).astype(F32), gram)
    step = 8
    blocks = [start[i : i + step] for i in range(0, k, step)]
    ids = lax.broadcasted_iota(jnp.int32, (step, 1), 0)
    for j in range(k):
        b, r = divmod(j, step)
        row = blocks[b][r : r + 1]
        scaled = row / row[:, k + j : k + j + 1]
        for i in range(b, k // step):
            column = blocks[i][:, k + j : k + j + 1]
            if i == b:
                column = jnp.where(ids > r, column, 0.0)
            blocks[i] = blocks[i] - column * scaled
    full = jnp.concatenate(blocks, axis=0)
    pivots = jnp.sum(jnp.where(lanes - k == row_ids, full, 0.0), axis=1, keepdims=True)
    return full / jnp.sqrt(pivots)


def kernel(
    n, owners, chunk, data, sketch, out, stage, drawn, high, low, small, parts, inbox, gathered, acc, grams, inverse,
    load_sem, drawn_sem, part_send, part_recv, gather_send, gather_recv, gram_send, gram_recv, inv_send, inv_recv,
):
    me, side = lax.axis_index("cells"), lax.axis_index("side")
    genes, width = data.shape[1:]
    k = sketch.shape[0]
    is_x, is_y = side == 0, side == 1
    barrier = pltpu.get_barrier_semaphore()

    def device(cell, which):
        return {"cells": cell, "side": which}

    def greet(s):
        cell = lax.rem(me + s + 1, n)
        pl.semaphore_signal(barrier, inc=1, device_id=device(cell, 1 - side), device_id_type=MESH)

        @pl.when(cell != me)
        def _():
            pl.semaphore_signal(barrier, inc=1, device_id=device(cell, side), device_id_type=MESH)

    def chunk_at(s):
        return lax.rem(me + 1 + s, owners)

    def start_of(c):
        return pl.multiple_of(jnp.minimum(c * chunk, genes - chunk), 8)

    def load(c):
        return pltpu.make_async_copy(data.at[0, pl.ds(start_of(c), chunk)], stage.at[c], load_sem.at[c])

    draw = pltpu.make_async_copy(sketch, drawn, drawn_sem)
    draw.start()
    each(owners, lambda s: load(chunk_at(s)).start())
    each(n, greet)

    def prepare(c):
        load(c).wait()
        rows = lax.broadcasted_iota(jnp.int32, (chunk, width), 0)
        value = jnp.where(rows >= c * chunk - start_of(c), stage[c], 0.0)
        high[c], low[c] = halves(value)

    def part_copy(c):
        return pltpu.make_async_remote_copy(
            src_ref=parts.at[c], dst_ref=inbox.at[me], send_sem=part_send.at[c], recv_sem=part_recv.at[me],
            device_id=device(c, 1 - side), device_id_type=MESH,
        )

    def part_arrival(i):
        return pltpu.make_async_remote_copy(
            src_ref=parts.at[0], dst_ref=inbox.at[i], send_sem=part_send.at[0], recv_sem=part_recv.at[i],
            device_id=device(i, 1 - side), device_id_type=MESH,
        )

    def gather_copy(cell, slot, which):
        return pltpu.make_async_remote_copy(
            src_ref=gathered.at[slot], dst_ref=gathered.at[slot], send_sem=gather_send.at[which],
            recv_sem=gather_recv.at[slot], device_id=device(cell, side), device_id_type=MESH,
        )

    def gram_copy(cell, slot, which):
        return pltpu.make_async_remote_copy(
            src_ref=grams.at[slot], dst_ref=grams.at[slot], send_sem=gram_send.at[which],
            recv_sem=gram_recv.at[slot], device_id=device(cell, side), device_id_type=MESH,
        )

    inverse_copy = pltpu.make_async_remote_copy(
        src_ref=inverse, dst_ref=inverse, send_sem=inv_send, recv_sem=inv_recv,
        device_id=device(me, 1 - side), device_id_type=MESH,
    )

    def scatter(s):
        c = chunk_at(s)
        parts[c] = dot3(small[...], high[c], low[c], NT)
        part_copy(c).start()

    draw.wait()

    @pl.when(is_x)
    def _():
        each(owners, lambda s: prepare(chunk_at(s)))

    @pl.when(is_y)
    def _():
        small[...] = stacked(drawn[...])
        prepare(chunk_at(0))

    pl.semaphore_wait(barrier, 2 * n - 1)

    @pl.when(is_y)
    def _():
        scatter(0)

        def onward(s):
            prepare(chunk_at(s + 1))
            scatter(s + 1)

        each(owners - 1, onward)

    @pl.when(me < owners)
    def _():
        first = lax.rem(me - 1 + n, n)
        part_arrival(first).wait_recv()
        gathered[me] = inbox[first]

        def add(s):
            i = lax.rem(me - 2 - s + 2 * n, n)
            part_arrival(i).wait_recv()
            gathered[me] += inbox[i]

        each(n - 1, add)
        each(n - 1, lambda s: gather_copy(lax.rem(me + 1 + s, n), me, s).start())

    acc[...] = jnp.zeros_like(acc)

    def collect(s):
        c = lax.rem(lax.rem(me, owners) - s + owners, owners)

        @pl.when(c != me)
        def _():
            gather_copy(me, c, 0).wait_recv()

        acc[...] += dot3(stacked(gathered[c]), high[c], low[c], NN)

    each(owners, collect)

    @pl.when(is_x)
    def _():
        range_rows = acc[...]
        small[...] = stacked(range_rows)
        grams[me] = lax.dot_general(
            range_rows, jnp.concatenate([range_rows, range_rows], axis=0), NT,
            precision=HIGHEST, preferred_element_type=F32,
        )
        each(n - 1, lambda s: gram_copy(lax.rem(me + 1 + s, n), me, s).start())
        each(owners, scatter)

        def arrive(s):
            gram_copy(me, lax.rem(me - 1 - s + n, n), 0).wait_recv()

        each(n - 1, arrive)
        inverse[...] = grams[0]

        def add(i):
            inverse[...] += grams[i + 1]

        each(n - 1, add)
        inverse[...] = inverse_factor(inverse[...])
        inverse_copy.start()

    @pl.when(is_y)
    def _():
        inverse_copy.wait_recv()

    scale = math.sqrt(width * n)
    factor = jnp.where(is_x, scale, 1.0 / scale).astype(F32)
    out[0] = factor * lax.dot_general(
        inverse[:, :k], acc[...], NN, precision=HIGHEST, preferred_element_type=F32
    )

    each(owners, lambda s: part_copy(chunk_at(s)).wait_send())

    @pl.when(me < owners)
    def _():
        each(n - 1, lambda s: gather_copy(lax.rem(me + 1 + s, n), me, s).wait_send())

    @pl.when(is_x)
    def _():
        each(n - 1, lambda s: gram_copy(lax.rem(me + 1 + s, n), me, s).wait_send())
        inverse_copy.wait_send()


def solution(mesh):
    n = mesh.shape["cells"]

    def per_device(datasets, sketch):
        genes, width = datasets.shape[1:]
        k = sketch.shape[0]
        chunk = 128 * -(-genes // (128 * n))
        owners = -(-genes // chunk)
        dma = pltpu.SemaphoreType.DMA
        return pl.pallas_call(
            functools.partial(kernel, n, owners, chunk),
            out_shape=jax.ShapeDtypeStruct((1, k, width), F32),
            in_specs=[pl.BlockSpec(memory_space=pl.ANY)] * 2,
            out_specs=pl.BlockSpec(memory_space=pltpu.VMEM),
            scratch_shapes=[
                pltpu.VMEM((owners, chunk, width), F32),
                pltpu.VMEM((k, width), F32),
                pltpu.VMEM((owners, chunk, width), BF16),
                pltpu.VMEM((owners, chunk, width), BF16),
                pltpu.VMEM((2 * k, width), BF16),
                pltpu.VMEM((owners, k, chunk), F32),
                pltpu.VMEM((n, k, chunk), F32),
                pltpu.VMEM((owners, k, chunk), F32),
                pltpu.VMEM((k, width), F32),
                pltpu.VMEM((n, k, 2 * k), F32),
                pltpu.VMEM((k, 2 * k), F32),
                dma((owners,)), dma,
                dma((owners,)), dma((n,)),
                dma((n,)), dma((owners,)),
                dma((n,)), dma((n,)),
                dma, dma,
            ],
            compiler_params=pltpu.CompilerParams(collective_id=0, has_side_effects=True),
            name="power_pass",
        )(datasets, sketch)

    spec = P("side", None, ("groups", "cells"))
    return jax.shard_map(
        per_device, mesh=mesh, in_specs=(spec, P(None, ("groups", "cells"))), out_specs=spec, check_vma=False
    )
```

```python
import functools
import math

import jax
import jax.numpy as jnp
from jax import lax
from jax.experimental import pallas as pl
from jax.experimental.pallas import tpu as pltpu
from jax.sharding import PartitionSpec as P

MESH = pl.DeviceIdType.MESH
F32, BF16 = jnp.float32, jnp.bfloat16
HIGHEST = lax.Precision.HIGHEST
NT = (((1,), (1,)), ((), ()))
NN = (((1,), (0,)), ((), ()))


def each(count, body):
    if count <= 8:
        for index in range(count):
            body(index)
    else:
        lax.fori_loop(0, count, lambda index, carry: (body(index), carry)[1], 0)


def flipped(cell, bits, count):
    bit = 1
    while bit < count:
        own = lax.rem(cell // bit, 2)
        cell = cell + (bits // bit % 2) * (bit - 2 * bit * own)
        bit *= 2
    return cell


def halves(value):
    high = value.astype(BF16)
    low = (value - high.astype(F32)).astype(BF16)
    return high, low


def stacked(value):
    return jnp.concatenate(halves(value), axis=0)


def dot3(small, high, low, dims):
    rows = small.shape[0] // 2
    both = lax.dot_general(small, high, dims, preferred_element_type=F32)
    rest = lax.dot_general(small[:rows], low, dims, preferred_element_type=F32)
    return both[:rows] + (both[rows:] + rest)


def inverse_factor(gram):
    k = gram.shape[0]
    row_ids = lax.broadcasted_iota(jnp.int32, gram.shape, 0)
    lanes = lax.broadcasted_iota(jnp.int32, gram.shape, 1)
    start = jnp.where(lanes < k, (lanes == row_ids).astype(F32), gram)
    step = 8
    blocks = [start[i : i + step] for i in range(0, k, step)]
    ids = lax.broadcasted_iota(jnp.int32, (step, 1), 0)
    for j in range(k):
        b, r = divmod(j, step)
        row = blocks[b][r : r + 1]
        scaled = row / row[:, k + j : k + j + 1]
        for i in range(b, k // step):
            column = blocks[i][:, k + j : k + j + 1]
            if i == b:
                column = jnp.where(ids > r, column, 0.0)
            blocks[i] = blocks[i] - column * scaled
    full = jnp.concatenate(blocks, axis=0)
    pivots = jnp.sum(jnp.where(lanes - k == row_ids, full, 0.0), axis=1, keepdims=True)
    return full / jnp.sqrt(pivots)


def kernel(
    n, owners, chunk, data, sketch, out, stage, drawn, high, low, small, parts, inbox, gathered, acc, grams, total, inverse,
    passing, load_sem, drawn_sem, pass_send, pass_recv, part_send, part_recv, gather_send, gather_recv, gram_send, gram_recv, inv_send, inv_recv,
):
    me, side = lax.axis_index("cells"), lax.axis_index("side")
    genes, width = data.shape[1:]
    k = sketch.shape[0]
    is_x, is_y = side == 0, side == 1
    barrier = pltpu.get_barrier_semaphore()

    def device(cell, which):
        return {"cells": cell, "side": which}

    def greet(s):
        cell = lax.rem(me + s + 1, n)
        pl.semaphore_signal(barrier, inc=1, device_id=device(cell, 1 - side), device_id_type=MESH)

        @pl.when(cell != me)
        def _():
            pl.semaphore_signal(barrier, inc=1, device_id=device(cell, side), device_id_type=MESH)

    relayed = owners == n == 8
    far, far_across = n // 2, n // 2 + 1

    def cell_at(s):
        return flipped(me, s, n) if relayed else lax.rem(me + s, n)

    relay_sums, relay_gathers = relayed, relayed
    part_order = sum_order = gather_order = collect_order = None
    if relayed:
        part_order = ((5, 6, 7, 2, 3, 1, 0, 4), (5, 2, 3, 6, 7, 1, 0, 4)) if relay_sums else (2, 3, 4, 5, 6, 7, 1, 0)
        sum_order = (0, 1, 2, 3, 6, 7, 4) if relay_sums else (0, 1, 2, 3, 4, 5, 6, 7)
        gather_order = ((4, 6, 7, 2, 3, 1), (4, 2, 3, 6, 7, 1)) if relay_gathers else (2, 3, 4, 5, 6, 7, 1)
        collect_order = (0, 1, 4, 2, 3, 6, 7, 5) if relay_gathers else (0, 1, 2, 3, 4, 5, 6, 7)

    def through(order, count, body, start=0):
        if order is None:
            each(count - start, lambda s: body(s + start))
        elif isinstance(order[0], tuple):
            inner = (me >= 2) & (me < 6)
            for test, own_order in zip((inner, jnp.logical_not(inner)), order):

                @pl.when(test)
                def _():
                    through(own_order, count, body, start)
        else:
            for s in order:
                body(s)

    def chunk_at(s):
        return cell_at(s) if relayed else lax.rem(me + 1 + s, owners)

    def start_of(c):
        return pl.multiple_of(jnp.minimum(c * chunk, genes - chunk), 8)

    def load(c):
        return pltpu.make_async_copy(data.at[0, pl.ds(start_of(c), chunk)], stage.at[c], load_sem.at[c])

    draw = pltpu.make_async_copy(sketch, drawn, drawn_sem)
    draw.start()
    through(part_order, owners, lambda s: load(chunk_at(s)).start())
    each(n, greet)

    def prepare(c):
        load(c).wait()
        rows = lax.broadcasted_iota(jnp.int32, (chunk, width), 0)
        value = jnp.where(rows >= c * chunk - start_of(c), stage[c], 0.0)
        high[c], low[c] = halves(value)

    def part_copy(c):
        return pltpu.make_async_remote_copy(
            src_ref=parts.at[c], dst_ref=inbox.at[me], send_sem=part_send.at[c], recv_sem=part_recv.at[me],
            device_id=device(c, 1 - side), device_id_type=MESH,
        )

    def part_arrival(i):
        return pltpu.make_async_remote_copy(
            src_ref=parts.at[0], dst_ref=inbox.at[i], send_sem=part_send.at[0], recv_sem=part_recv.at[i],
            device_id=device(i, 1 - side), device_id_type=MESH,
        )

    def gather_copy(cell, slot, which):
        return pltpu.make_async_remote_copy(
            src_ref=gathered.at[slot], dst_ref=gathered.at[slot], send_sem=gather_send.at[which],
            recv_sem=gather_recv.at[slot], device_id=device(cell, side), device_id_type=MESH,
        )

    def gram_copy(cell, slot, which):
        return pltpu.make_async_remote_copy(
            src_ref=grams.at[slot], dst_ref=grams.at[slot], send_sem=gram_send.at[which],
            recv_sem=gram_recv.at[slot], device_id=device(cell, side), device_id_type=MESH,
        )

    inverse_copy = pltpu.make_async_remote_copy(
        src_ref=inverse, dst_ref=inverse, send_sem=inv_send, recv_sem=inv_recv,
        device_id=device(me, 1 - side), device_id_type=MESH,
    )

    def work_out(s):
        c = chunk_at(s)
        parts[c] = dot3(small[...], high[c], low[c], NT)

    relay_part = pltpu.make_async_remote_copy(
        src_ref=parts.at[cell_at(far_across)], dst_ref=passing, send_sem=pass_send, recv_sem=pass_recv,
        device_id=device(cell_at(1), side), device_id_type=MESH,
    )

    def send(s):
        if relay_sums and s == far_across:
            relay_part.start()
            return
        if relay_sums and s == far:
            relay_part.wait_recv()
            parts[chunk_at(s)] += passing[...]
        part_copy(chunk_at(s)).start()

    def scatter(s):
        work_out(s)
        send(s)

    def prepare_and_work_out(s):
        prepare(chunk_at(s))
        work_out(s)

    draw.wait()

    @pl.when(is_x)
    def _():
        through(part_order, owners, lambda s: prepare(chunk_at(s)))

    @pl.when(is_y)
    def _():
        small[...] = stacked(drawn[...])
        through(part_order, owners, prepare_and_work_out)

    pl.semaphore_wait(barrier, 2 * n - 1)

    @pl.when(is_y)
    def _():
        through(part_order, owners, send)

    @pl.when(me < owners)
    def _():
        def add(s):
            i = cell_at(s)
            part_arrival(i).wait_recv()
            if isinstance(s, int) and s == 0:
                gathered[me] = inbox[i]
            else:
                gathered[me] += inbox[i]

        if relayed:
            through(sum_order, n, add)
        else:
            add(0)
            each(n - 1, lambda s: add(s + 1))
        through(gather_order, n, lambda s: gather_copy(cell_at(s), me, s).start(), 1)

    acc[...] = jnp.zeros_like(acc)

    relay_gather = gather_copy(cell_at(1), cell_at(far), 0) if relay_gathers else None

    def collect(s):
        c = cell_at(s) if relayed else lax.rem(lax.rem(me, owners) - s + owners, owners)

        @pl.when(c != me)
        def _():
            gather_copy(me, c, 0).wait_recv()

        if relay_gathers and s == far:
            relay_gather.start()
        acc[...] += dot3(stacked(gathered[c]), high[c], low[c], NN)

    through(collect_order, owners, collect)

    @pl.when(is_x)
    def _():
        range_rows = acc[...]
        small[...] = stacked(range_rows)
        twice = lax.dot_general(
            range_rows, jnp.concatenate([range_rows, range_rows], axis=0), NT,
            precision=HIGHEST, preferred_element_type=F32,
        )
        left = lax.broadcasted_iota(jnp.int32, grams.shape[1:], 1) < k
        grams[me] = jnp.where(left, twice[: k // 2], twice[k // 2 :])
        each(n - 1, lambda s: gram_copy(lax.rem(me + 1 + s, n), me, s).start())
        through(part_order, owners, scatter)

        def arrive(s):
            gram_copy(me, lax.rem(me - 1 - s + n, n), 0).wait_recv()

        each(n - 1, arrive)
        total[...] = grams[0]

        def add(i):
            total[...] += grams[i + 1]

        each(n - 1, add)
        bottom = total[...]
        gram = jnp.concatenate([pltpu.roll(bottom, k, axis=1), bottom], axis=0)
        inverse[...] = inverse_factor(gram)
        inverse_copy.start()

    @pl.when(is_y)
    def _():
        inverse_copy.wait_recv()

    scale = math.sqrt(width * n)
    factor = jnp.where(is_x, scale, 1.0 / scale).astype(F32)
    out[0] = factor * lax.dot_general(
        inverse[:, :k], acc[...], NN, precision=HIGHEST, preferred_element_type=F32
    )

    through(part_order, owners, lambda s: (relay_part if relay_sums and s == far_across else part_copy(chunk_at(s))).wait_send())

    @pl.when(me < owners)
    def _():
        through(gather_order, n, lambda s: gather_copy(cell_at(s), me, s).wait_send(), 1)

    if relay_gathers:
        relay_gather.wait_send()

    @pl.when(is_x)
    def _():
        each(n - 1, lambda s: gram_copy(lax.rem(me + 1 + s, n), me, s).wait_send())
        inverse_copy.wait_send()


def solution(mesh):
    n = mesh.shape["cells"]

    def per_device(datasets, sketch):
        genes, width = datasets.shape[1:]
        k = sketch.shape[0]
        chunk = 128 * -(-genes // (128 * n))
        owners = -(-genes // chunk)
        dma = pltpu.SemaphoreType.DMA
        return pl.pallas_call(
            functools.partial(kernel, n, owners, chunk),
            out_shape=jax.ShapeDtypeStruct((1, k, width), F32),
            in_specs=[pl.BlockSpec(memory_space=pl.ANY)] * 2,
            out_specs=pl.BlockSpec(memory_space=pltpu.VMEM),
            scratch_shapes=[
                pltpu.VMEM((owners, chunk, width), F32),
                pltpu.VMEM((k, width), F32),
                pltpu.VMEM((owners, chunk, width), BF16),
                pltpu.VMEM((owners, chunk, width), BF16),
                pltpu.VMEM((2 * k, width), BF16),
                pltpu.VMEM((owners, k, chunk), F32),
                pltpu.VMEM((n, k, chunk), F32),
                pltpu.VMEM((owners, k, chunk), F32),
                pltpu.VMEM((k, width), F32),
                pltpu.VMEM((n, k // 2, 2 * k), F32),
                pltpu.VMEM((k // 2, 2 * k), F32),
                pltpu.VMEM((k, 2 * k), F32),
                pltpu.VMEM((k, chunk), F32),
                dma((owners,)), dma, dma, dma,
                dma((owners,)), dma((n,)),
                dma((n,)), dma((owners,)),
                dma((n,)), dma((n,)),
                dma, dma,
            ],
            compiler_params=pltpu.CompilerParams(collective_id=0, has_side_effects=True),
            name="power_pass",
        )(datasets, sketch)

    spec = P("side", None, ("groups", "cells"))
    return jax.shard_map(
        per_device, mesh=mesh, in_specs=(spec, P(None, ("groups", "cells"))), out_specs=spec, check_vma=False
    )
```

```python
import functools
import math

import jax
import jax.numpy as jnp
from jax import lax
from jax.experimental import pallas as pl
from jax.experimental.pallas import tpu as pltpu
from jax.sharding import PartitionSpec as P

MESH = pl.DeviceIdType.MESH
F32, BF16 = jnp.float32, jnp.bfloat16
HIGHEST = lax.Precision.HIGHEST
NT = (((1,), (1,)), ((), ()))
NN = (((1,), (0,)), ((), ()))


def each(count, body):
    if count <= 8:
        for index in range(count):
            body(index)
    else:
        lax.fori_loop(0, count, lambda index, carry: (body(index), carry)[1], 0)


def flipped(cell, bits, count):
    bit = 1
    while bit < count:
        own = lax.rem(cell // bit, 2)
        cell = cell + (bits // bit % 2) * (bit - 2 * bit * own)
        bit *= 2
    return cell


def halves(value):
    high = value.astype(BF16)
    low = (value - high.astype(F32)).astype(BF16)
    return high, low


def stacked(value):
    return jnp.concatenate(halves(value), axis=0)


def dot3(small, high, low, dims):
    rows = small.shape[0] // 2
    both = lax.dot_general(small, high, dims, preferred_element_type=F32)
    rest = lax.dot_general(small[:rows], low, dims, preferred_element_type=F32)
    return both[:rows] + (both[rows:] + rest)


def inverse_factor(gram):
    k = gram.shape[0]
    row_ids = lax.broadcasted_iota(jnp.int32, gram.shape, 0)
    lanes = lax.broadcasted_iota(jnp.int32, gram.shape, 1)
    start = jnp.where(lanes < k, (lanes == row_ids).astype(F32), gram)
    step = 8
    blocks = [start[i : i + step] for i in range(0, k, step)]
    ids = lax.broadcasted_iota(jnp.int32, (step, 1), 0)
    for j in range(k):
        b, r = divmod(j, step)
        row = blocks[b][r : r + 1]
        scaled = row / row[:, k + j : k + j + 1]
        for i in range(b, k // step):
            column = blocks[i][:, k + j : k + j + 1]
            if i == b:
                column = jnp.where(ids > r, column, 0.0)
            blocks[i] = blocks[i] - column * scaled
    full = jnp.concatenate(blocks, axis=0)
    pivots = jnp.sum(jnp.where(lanes - k == row_ids, full, 0.0), axis=1, keepdims=True)
    return full / jnp.sqrt(pivots)


def kernel(
    n, owners, chunk, data, sketch, out, stage, drawn, high, low, small, parts, inbox, gathered, acc, grams, total, inverse,
    passing, load_sem, drawn_sem, pass_send, pass_recv, part_send, part_recv, gather_send, gather_recv, gram_send, gram_recv, inv_send, inv_recv,
):
    me, side = lax.axis_index("cells"), lax.axis_index("side")
    genes, width = data.shape[1:]
    k = sketch.shape[0]
    is_x, is_y = side == 0, side == 1
    barrier = pltpu.get_barrier_semaphore()

    def device(cell, which):
        return {"cells": cell, "side": which}

    def greet(s):
        cell = lax.rem(me + s + 1, n)
        pl.semaphore_signal(barrier, inc=1, device_id=device(cell, 1 - side), device_id_type=MESH)

        @pl.when(cell != me)
        def _():
            pl.semaphore_signal(barrier, inc=1, device_id=device(cell, side), device_id_type=MESH)

    relayed = owners == n == 8
    far, far_across = n // 2, n // 2 + 1

    def cell_at(s):
        return flipped(me, s, n) if relayed else lax.rem(me + s, n)

    relay_sums, relay_gathers = relayed, relayed
    part_order = sum_order = gather_order = collect_order = None
    if relayed:
        part_order = ((5, 6, 7, 2, 3, 1, 0, 4), (5, 2, 3, 6, 7, 1, 0, 4)) if relay_sums else (2, 3, 4, 5, 6, 7, 1, 0)
        sum_order = (0, 1, 2, 3, 6, 7, 4) if relay_sums else (0, 1, 2, 3, 4, 5, 6, 7)
        gather_order = ((4, 6, 7, 2, 3, 1), (4, 2, 3, 6, 7, 1)) if relay_gathers else (2, 3, 4, 5, 6, 7, 1)
        collect_order = (0, 1, 4, 2, 3, 6, 7, 5) if relay_gathers else (0, 1, 2, 3, 4, 5, 6, 7)

    def through(order, count, body, start=0):
        if order is None:
            each(count - start, lambda s: body(s + start))
        elif isinstance(order[0], tuple):
            inner = (me >= 2) & (me < 6)
            for test, own_order in zip((inner, jnp.logical_not(inner)), order):

                @pl.when(test)
                def _():
                    through(own_order, count, body, start)
        else:
            for s in order:
                body(s)

    def chunk_at(s):
        return cell_at(s) if relayed else lax.rem(me + 1 + s, owners)

    def start_of(c):
        return pl.multiple_of(jnp.minimum(c * chunk, genes - chunk), 8)

    def load(c):
        return pltpu.make_async_copy(data.at[0, pl.ds(start_of(c), chunk)], stage.at[c], load_sem.at[c])

    draw = pltpu.make_async_copy(sketch, drawn, drawn_sem)
    draw.start()
    through(part_order, owners, lambda s: load(chunk_at(s)).start())
    each(n, greet)

    def prepare(c):
        load(c).wait()
        rows = lax.broadcasted_iota(jnp.int32, (chunk, width), 0)
        value = jnp.where(rows >= c * chunk - start_of(c), stage[c], 0.0)
        high[c], low[c] = halves(value)

    def part_copy(c):
        return pltpu.make_async_remote_copy(
            src_ref=parts.at[c], dst_ref=inbox.at[me], send_sem=part_send.at[c], recv_sem=part_recv.at[me],
            device_id=device(c, 1 - side), device_id_type=MESH,
        )

    def part_arrival(i):
        return pltpu.make_async_remote_copy(
            src_ref=parts.at[0], dst_ref=inbox.at[i], send_sem=part_send.at[0], recv_sem=part_recv.at[i],
            device_id=device(i, 1 - side), device_id_type=MESH,
        )

    def gather_copy(cell, slot, which):
        return pltpu.make_async_remote_copy(
            src_ref=gathered.at[slot], dst_ref=gathered.at[slot], send_sem=gather_send.at[which],
            recv_sem=gather_recv.at[slot], device_id=device(cell, side), device_id_type=MESH,
        )

    def gram_copy(cell, slot, which):
        return pltpu.make_async_remote_copy(
            src_ref=grams.at[slot], dst_ref=grams.at[slot], send_sem=gram_send.at[which],
            recv_sem=gram_recv.at[slot], device_id=device(cell, side), device_id_type=MESH,
        )

    inverse_copy = pltpu.make_async_remote_copy(
        src_ref=inverse, dst_ref=inverse, send_sem=inv_send, recv_sem=inv_recv,
        device_id=device(me, 1 - side), device_id_type=MESH,
    )

    def work_out(s):
        c = chunk_at(s)
        parts[c] = dot3(small[...], high[c], low[c], NT)

    relay_part = pltpu.make_async_remote_copy(
        src_ref=parts.at[cell_at(far_across)], dst_ref=passing, send_sem=pass_send, recv_sem=pass_recv,
        device_id=device(cell_at(1), side), device_id_type=MESH,
    )

    def send(s):
        if relay_sums and s == far_across:
            relay_part.start()
            return
        if relay_sums and s == far:
            relay_part.wait_recv()
            parts[chunk_at(s)] += passing[...]
        part_copy(chunk_at(s)).start()

    def scatter(s):
        work_out(s)
        send(s)

    def prepare_and_work_out(s):
        prepare(chunk_at(s))
        work_out(s)

    draw.wait()

    @pl.when(is_x)
    def _():
        through(part_order, owners, lambda s: prepare(chunk_at(s)))

    @pl.when(is_y)
    def _():
        small[...] = stacked(drawn[...])
        through(part_order, owners, prepare_and_work_out)

    pl.semaphore_wait(barrier, 2 * n - 1)

    @pl.when(is_y)
    def _():
        through(part_order, owners, send)

    @pl.when(me < owners)
    def _():
        def add(s):
            i = cell_at(s)
            part_arrival(i).wait_recv()
            if isinstance(s, int) and s == 0:
                gathered[me] = inbox[i]
            else:
                gathered[me] += inbox[i]

        if relayed:
            through(sum_order, n, add)
        else:
            add(0)
            each(n - 1, lambda s: add(s + 1))
        through(gather_order, n, lambda s: gather_copy(cell_at(s), me, s).start(), 1)

    acc[...] = jnp.zeros_like(acc)

    relay_gather = gather_copy(cell_at(1), cell_at(far), 0) if relay_gathers else None

    def collect(s):
        c = cell_at(s) if relayed else lax.rem(lax.rem(me, owners) - s + owners, owners)

        @pl.when(c != me)
        def _():
            gather_copy(me, c, 0).wait_recv()

        if relay_gathers and s == far:
            relay_gather.start()
        acc[...] += dot3(stacked(gathered[c]), high[c], low[c], NN)

    through(collect_order, owners, collect)

    @pl.when(is_x)
    def _():
        range_rows = acc[...]
        small[...] = stacked(range_rows)
        twice = lax.dot_general(
            range_rows, jnp.concatenate([range_rows, range_rows], axis=0), NT,
            precision=HIGHEST, preferred_element_type=F32,
        )
        left = lax.broadcasted_iota(jnp.int32, grams.shape[1:], 1) < k
        grams[me] = jnp.where(left, twice[: k // 2], twice[k // 2 :])
        each(n - 1, lambda s: gram_copy(lax.rem(me + 1 + s, n), me, s).start())
        through(part_order, owners, scatter)

        def arrive(s):
            gram_copy(me, lax.rem(me - 1 - s + n, n), 0).wait_recv()

        each(n - 1, arrive)
        total[...] = grams[0]

        def add(i):
            total[...] += grams[i + 1]

        each(n - 1, add)
        bottom = total[...]
        gram = jnp.concatenate([pltpu.roll(bottom, k, axis=1), bottom], axis=0)
        inverse[...] = inverse_factor(gram)
        inverse_copy.start()

    @pl.when(is_y)
    def _():
        inverse_copy.wait_recv()

    scale = math.sqrt(width * n)
    factor = jnp.where(is_x, scale, 1.0 / scale).astype(F32)
    out[0] = factor * dot3(stacked(inverse[:, :k]), *halves(acc[...]), NN)

    through(part_order, owners, lambda s: (relay_part if relay_sums and s == far_across else part_copy(chunk_at(s))).wait_send())

    @pl.when(me < owners)
    def _():
        through(gather_order, n, lambda s: gather_copy(cell_at(s), me, s).wait_send(), 1)

    if relay_gathers:
        relay_gather.wait_send()

    @pl.when(is_x)
    def _():
        each(n - 1, lambda s: gram_copy(lax.rem(me + 1 + s, n), me, s).wait_send())
        inverse_copy.wait_send()


def solution(mesh):
    n = mesh.shape["cells"]

    def per_device(datasets, sketch):
        genes, width = datasets.shape[1:]
        k = sketch.shape[0]
        chunk = 128 * -(-genes // (128 * n))
        owners = -(-genes // chunk)
        dma = pltpu.SemaphoreType.DMA
        return pl.pallas_call(
            functools.partial(kernel, n, owners, chunk),
            out_shape=jax.ShapeDtypeStruct((1, k, width), F32),
            in_specs=[pl.BlockSpec(memory_space=pl.ANY)] * 2,
            out_specs=pl.BlockSpec(memory_space=pltpu.VMEM),
            scratch_shapes=[
                pltpu.VMEM((owners, chunk, width), F32),
                pltpu.VMEM((k, width), F32),
                pltpu.VMEM((owners, chunk, width), BF16),
                pltpu.VMEM((owners, chunk, width), BF16),
                pltpu.VMEM((2 * k, width), BF16),
                pltpu.VMEM((owners, k, chunk), F32),
                pltpu.VMEM((n, k, chunk), F32),
                pltpu.VMEM((owners, k, chunk), F32),
                pltpu.VMEM((k, width), F32),
                pltpu.VMEM((n, k // 2, 2 * k), F32),
                pltpu.VMEM((k // 2, 2 * k), F32),
                pltpu.VMEM((k, 2 * k), F32),
                pltpu.VMEM((k, chunk), F32),
                dma((owners,)), dma, dma, dma,
                dma((owners,)), dma((n,)),
                dma((n,)), dma((owners,)),
                dma((n,)), dma((n,)),
                dma, dma,
            ],
            compiler_params=pltpu.CompilerParams(collective_id=0, has_side_effects=True),
            name="power_pass",
        )(datasets, sketch)

    spec = P("side", None, ("groups", "cells"))
    return jax.shard_map(
        per_device, mesh=mesh, in_specs=(spec, P(None, ("groups", "cells"))), out_specs=spec, check_vma=False
    )
```
